32 devices in a mesh: up: 8 (over y, x, core), dn: 4 (over z).
Axes of the slice: x: 2, y: 2, z: 4, core: 2. Of those that a mesh axis runs over, the one named last changes fastest.
Arguments:
- start_vector: bfloat16 [13312, 13312], P('up', 'dn'), may hold values from -6 to 6
- hop_tiles: bfloat16 [104, 5, 128, 128], replicated, may hold values from -0.5 to 0.5
- tile_columns: int32 [104, 5], replicated, may hold values from 0 to 103, as said below
- tile_signs: int32 [104, 5], replicated, may hold values from 0 to 1
- occupation: int32 [16, 13312], replicated, may hold values from 0 to 1, as said below
Outputs:
- next_vector: bfloat16 [13312, 13312], P('up', 'dn')
- alphas: float32 [2], replicated
- betas: float32 [2], replicated
The draws below stay inside these ranges and needn't reach their ends.
Inputs may be any that keep to these rules, and one draw needn't show every extreme that they name: Each row of tile_columns names 5 different tile columns. Every column of occupation holds exactly 8 ones.
All inputs are finite; a program needn't handle non-finite values.
Results may differ from the reference program's by a relative error of at most 0.0065.
Values may be sent and summed in bfloat16 or wider, within the bound.
A program may use at most 256 MiB of HBM per device.

```python
import jax
import jax.numpy as jnp
from jax import lax

DETS = 13312
SITES = 16
TILE = 128
TILE_K = 5
STEPS = 2
TILES = 104


def draw_tile_columns(key, part):
    scores = jax.random.randint(key, (TILES, TILES), 0, 1 << 20) * TILES + jnp.arange(TILES, dtype=jnp.int32)[None, :]
    order = jnp.argsort(scores, axis=1)
    return order[:, :TILE_K].astype(jnp.int32)


def draw_occupation(key, part):
    scores = jax.random.randint(key, (DETS, SITES), 0, 1 << 20) * SITES + jnp.arange(SITES, dtype=jnp.int32)[None, :]
    ranks = jnp.argsort(jnp.argsort(scores, axis=1), axis=1)
    filled = (ranks < SITES // 2).astype(jnp.int32)
    return filled.T


def with_ends(drawn, key, smallest, high):
    dims = drawn.shape
    index_at = [jax.random.randint(jax.random.fold_in(key, axis), (), 0, dims[axis]) for axis in range(len(dims))]
    drawn = drawn.at[tuple(index_at)].set(smallest)
    longest = dims.index(max(dims))
    index_at[longest] = (index_at[longest] + 1) % dims[longest]
    return drawn.at[tuple(index_at)].set(high)


def block_scale(key, dims, shards, smallest, high):
    level = 1.0
    for dim, blocks in shards:
        draws = jax.random.uniform(jax.random.fold_in(jax.random.fold_in(key, 6), dim), (blocks,), jnp.float32, smallest / len(shards), high / len(shards))
        level = level * jnp.repeat(jnp.exp(draws), dims[dim] // blocks).reshape((-1,) + (1,) * (len(dims) - 1 - dim))
    return level


def bell_draw(rng, shape, spread, most, pieces=(), held_as=jnp.bfloat16):
    loudness = block_scale(rng, shape, pieces, -0.22, 0.18) if pieces else 1.0
    entries = jax.random.normal(rng, shape, jnp.float32) * spread * loudness
    return jnp.minimum(jnp.maximum(entries, -most), most).astype(held_as)


def setup_inputs(seed: int = 0) -> dict:
    seeds = jax.random.split(jax.random.key(seed), 6)
    start_vector = bell_draw(seeds[0], (DETS, DETS), 1.0, 6.0, ((0, 8), (1, 4)))
    hop_tiles = bell_draw(seeds[1], (TILES, TILE_K, TILE, TILE), TILE ** -0.5, 0.5)
    tile_columns = draw_tile_columns(jax.random.fold_in(seeds[5], 71), 0)
    tile_signs = with_ends(jax.random.randint(seeds[3], (TILES, TILE_K), 0, 2), jax.random.fold_in(seeds[3], 1), 0, 1).astype(jnp.int32)
    occupation = draw_occupation(jax.random.fold_in(seeds[5], 71), 0)
    return {"start_vector": start_vector, "hop_tiles": hop_tiles, "tile_columns": tile_columns, "tile_signs": tile_signs, "occupation": occupation}


coupling = 4.0

def hop_last(matrix, signed_wide, tile_columns):

    def one_block(part):
        cube = part.reshape(part.shape[0], TILES, TILE)
        picked = cube[:, tile_columns].astype(jnp.float32)
        result = jnp.einsum('ikab,mikb->mia', signed_wide, picked, precision=lax.Precision.HIGHEST)
        return result.reshape(part.shape)
    blocks = matrix.reshape(-1, 512, matrix.shape[1])
    return lax.map(one_block, blocks).reshape(matrix.shape)

def reference(start_vector, hop_tiles, tile_columns, tile_signs, occupation):
    signed = hop_tiles * (1 - 2 * tile_signs).astype(jnp.bfloat16)[:, :, None, None]
    signed_wide = signed.astype(jnp.float32)
    occupied = occupation.astype(jnp.bfloat16)
    diagonal = coupling * jnp.dot(occupied.T, occupied, preferred_element_type=jnp.float32)
    vector = start_vector.astype(jnp.float32)
    total = jnp.sum(vector * vector)
    vector = vector / jnp.maximum(jnp.sqrt(total), 1.0)
    previous = jnp.zeros_like(vector)
    beta_value = jnp.float32(0.0)
    alpha_list = []
    beta_list = []
    for iteration in range(STEPS):
        rounded = vector.astype(jnp.bfloat16)
        hopped_up = hop_last(rounded.T, signed_wide, tile_columns).T.astype(jnp.bfloat16)
        hopped_down = hop_last(rounded, signed_wide, tile_columns).astype(jnp.bfloat16)
        work = hopped_up.astype(jnp.float32) + hopped_down.astype(jnp.float32) + diagonal * vector - beta_value * previous
        intersect = jnp.sum(work * vector)
        work = work - intersect * vector
        residual = jnp.sum(work * work)
        beta_value = jnp.sqrt(jnp.maximum(residual, 1.0))
        previous = vector
        vector = work / beta_value
        alpha_list.append(intersect)
        beta_list.append(beta_value)
    return (vector.astype(jnp.bfloat16), jnp.stack(alpha_list), jnp.stack(beta_list))
```

```python
import functools

import jax
import jax.numpy as jnp
from jax import lax
from jax.experimental import pallas as pl
from jax.experimental.pallas import tpu as pltpu
from jax.sharding import PartitionSpec as P

STEPS = 2


coupling = 4.0


def hop_kernel(tile_k, tile, group, parts_tiles, columns_ref, x_ref, tiles_ref, out_ref):
    first = pl.program_id(0) * group

    def one_tile(t, carry):
        picked = []
        for k in range(tile_k):
            column = columns_ref[(first + t) * tile_k + k]
            at = pl.multiple_of(lax.rem(column, parts_tiles) * tile, tile)
            picked.append(x_ref[lax.div(column, parts_tiles), :, pl.ds(at, tile)])
        left = jnp.concatenate(picked, axis=1)
        result = jnp.dot(left, tiles_ref[t], preferred_element_type=jnp.float32)
        out_ref[0, :, pl.ds(pl.multiple_of(t * tile, tile), tile)] = result.astype(jnp.bfloat16)
        return carry

    lax.fori_loop(0, group, one_tile, 0)


def hop_blocks(x, stacked, columns, tile_k):
    parts, rows, width = x.shape
    tiles, depth, tile = stacked.shape
    if width % tile:
        joined = x.transpose(1, 0, 2).reshape(1, rows, parts * width)
        hopped = hop_blocks(joined, stacked, columns, tile_k)
        return hopped.reshape(rows, parts, width).transpose(1, 0, 2)
    parts_tiles = width // tile
    group = max(d for d in range(1, 17) if parts_tiles % d == 0)
    per_part = parts_tiles // group
    return pl.pallas_call(
        functools.partial(hop_kernel, tile_k, tile, group, parts_tiles),
        grid_spec=pltpu.PrefetchScalarGridSpec(
            num_scalar_prefetch=1,
            grid=(tiles // group,),
            in_specs=[
                pl.BlockSpec((parts, rows, width), lambda i, c: (0, 0, 0)),
                pl.BlockSpec((group, depth, tile), lambda i, c: (i, 0, 0)),
            ],
            out_specs=pl.BlockSpec(
                (1, rows, group * tile), lambda i, c: (i // per_part, 0, i % per_part)
            ),
        ),
        out_shape=jax.ShapeDtypeStruct(x.shape, jnp.bfloat16),
        compiler_params=pltpu.CompilerParams(vmem_limit_bytes=56 * 1024 * 1024),
        cost_estimate=pl.CostEstimate(
            flops=2 * rows * tiles * depth * tile,
            bytes_accessed=4 * rows * parts * width + 2 * tiles * depth * tile,
            transcendentals=0,
        ),
    )(columns, x, stacked)


def body(start_vector, hop_tiles, tile_columns, tile_signs, occupation):
    tiles, tile_k, tile, _ = hop_tiles.shape
    signed = hop_tiles * (1 - 2 * tile_signs).astype(jnp.bfloat16)[:, :, None, None]
    stacked = signed.transpose(0, 1, 3, 2).reshape(tiles, tile_k * tile, tile)
    columns = tile_columns.reshape(-1)
    block_rows, block_cols = start_vector.shape
    count_up = lax.axis_size("up")
    count_down = lax.axis_size("dn")
    row_start = lax.axis_index("up") * block_rows
    col_start = lax.axis_index("dn") * block_cols
    occ_rows = lax.dynamic_slice_in_dim(occupation, row_start, block_rows, 1).astype(jnp.bfloat16)
    occ_cols = lax.dynamic_slice_in_dim(occupation, col_start, block_cols, 1).astype(jnp.bfloat16)
    diagonal = (
        coupling * jnp.einsum("sa,sb->ab", occ_rows, occ_cols, preferred_element_type=jnp.float32)
    ).astype(jnp.bfloat16)
    total = lax.psum(jnp.sum(jnp.square(start_vector.astype(jnp.float32))), ("up", "dn"))
    scale = 1.0 / jnp.maximum(jnp.sqrt(total), 1.0)
    vector = start_vector.astype(jnp.float32) * scale
    length = total / jnp.maximum(total, 1.0)
    previous = None
    beta_value = None
    alpha_list = []
    beta_list = []
    for iteration in range(STEPS):
        rounded = start_vector if iteration == 0 else vector.astype(jnp.bfloat16)
        down = rounded.reshape(count_down, block_rows // count_down, block_cols)
        up = rounded.T.reshape(count_up, block_cols // count_up, block_rows)
        down = lax.all_to_all(down, "dn", 0, 0, tiled=True)
        up = lax.all_to_all(up, "up", 0, 0, tiled=True)
        down = hop_blocks(down, stacked, columns, tile_k)
        down = lax.all_to_all(down, "dn", 0, 0, tiled=True)
        up = hop_blocks(up, stacked, columns, tile_k)
        up = lax.all_to_all(up, "up", 0, 0, tiled=True)
        hopped_down = down.reshape(block_rows, block_cols)
        hopped_up = up.reshape(block_cols, block_rows).T
        hopped = hopped_up.astype(jnp.float32) + hopped_down.astype(jnp.float32)
        if iteration == 0:
            work = hopped * scale + diagonal * vector
        else:
            work = hopped + diagonal * vector - beta_value * previous
        intersect, square = lax.psum((jnp.sum(work * vector), jnp.sum(work * work)), ("up", "dn"))
        work = work - intersect * vector
        residual = square - 2.0 * intersect * intersect + intersect * intersect * length
        beta_value = jnp.sqrt(jnp.maximum(residual, 1.0))
        length = residual / jnp.maximum(residual, 1.0)
        previous = vector
        vector = work / beta_value
        alpha_list.append(intersect)
        beta_list.append(beta_value)
    final = vector.astype(jnp.bfloat16)
    return (final, jnp.stack(alpha_list), jnp.stack(beta_list))


MESH = pl.DeviceIdType.MESH
ANY = pl.ANY


def remote(src, dst, send_sem, recv_sem, axis, peer):
    return pltpu.make_async_remote_copy(
        src_ref=src,
        dst_ref=dst,
        send_sem=send_sem,
        recv_sem=recv_sem,
        device_id={axis: peer},
        device_id_type=MESH,
    )


def reduce_all(n_up, n_dn, me_up, me_dn, mine, z_slots, up_slots, sems):
    z_send, z_recv, up_send, up_recv = sems
    z_slots[me_dn] = mine[...]
    copies = []
    for d in range(1, n_dn):
        peer = lax.rem(me_dn + d, n_dn)
        copy = remote(mine, z_slots.at[me_dn], z_send.at[d - 1], z_recv.at[me_dn], "dn", peer)
        copy.start()
        copies.append(copy)
    for d in range(1, n_dn):
        peer = lax.rem(me_dn + d, n_dn)
        remote(mine, z_slots.at[peer], z_send.at[d - 1], z_recv.at[peer], "dn", peer).wait_recv()
    for copy in copies:
        copy.wait_send()
    mine[...] = jnp.sum(z_slots[...], axis=0)
    up_slots[me_up] = mine[...]
    copies = []
    for d in range(1, n_up):
        peer = lax.rem(me_up + d, n_up)
        copy = remote(mine, up_slots.at[me_up], up_send.at[d - 1], up_recv.at[me_up], "up", peer)
        copy.start()
        copies.append(copy)
    for d in range(1, n_up):
        peer = lax.rem(me_up + d, n_up)
        remote(mine, up_slots.at[peer], up_send.at[d - 1], up_recv.at[peer], "up", peer).wait_recv()
    for copy in copies:
        copy.wait_send()
    return jnp.sum(up_slots[...], axis=0)


def fold(x):
    return jnp.sum(x.reshape(-1, 8, x.shape[-1]), axis=0)


def kernel(
    dims, columns, signs, v, tiles, occ_all, occ_mine, rows_t, cols_t,
    m_out, w_out, sigma_out, gram_out,
    d0, s0, u0, r0, x1, x2, dn1, s1, u2, g2, d2, vt, dt, r2,
    x, y, w, a, b, staged, flat, turned, made, first, last, z_first, up_first, z_last, up_last,
    local, stage_sem, strip_sem, made_sem, a_send, a_recv, b_send, b_recv, c_send, c_recv,
    p_send, p_recv, q_send, q_recv, t_send, t_recv, o_send, o_recv, first_sems, last_sems,
):
    n_up, n_dn, count, tile_k, tile, group, spans = dims
    rows, cols = v.shape
    half = cols // 2
    wide_tiles = cols // tile
    tall_tiles = rows // tile
    half_tiles = wide_tiles // 2
    piece = x.shape[1]
    me_up = lax.axis_index("up")
    me_dn = lax.axis_index("dn")

    barrier = pltpu.get_barrier_semaphore()
    for d in range(1, n_dn):
        pl.semaphore_signal(
            barrier, inc=1, device_id={"dn": lax.rem(me_dn + d, n_dn)}, device_id_type=MESH
        )
    for d in range(1, n_up):
        pl.semaphore_signal(
            barrier, inc=1, device_id={"up": lax.rem(me_up + d, n_up)}, device_id_type=MESH
        )
    pl.semaphore_wait(barrier, n_dn + n_up - 2)

    def lanes(start, size):
        return pl.ds(pl.multiple_of(start, tile), size)

    def subs(start, size):
        return pl.ds(pl.multiple_of(start, 8), size)

    def peers(axis):
        n, me = (n_dn, me_dn) if axis == "dn" else (n_up, me_up)
        return [lax.rem(me + d, n) for d in range(1, n)]

    started = []

    def launch(copies):
        for copy in copies:
            copy.start()
        started.extend(copies)

    def arrive(copies):
        for copy in copies:
            copy.wait_recv()

    def z_in(c, receiving):
        return [
            remote(
                v.at[subs(peer * 2 * piece + c * piece, piece), :],
                x1.at[c, :, lanes((peer if receiving else me_dn) * cols, cols)],
                a_send.at[c, k], a_recv.at[c, peer if receiving else me_dn], "dn", peer,
            )
            for k, peer in enumerate(peers("dn"))
        ]

    def z_out(source, target, send, recv, span, slot, c, receiving):
        low, high = span
        return [
            remote(
                source.at[c, pl.ds(peer * wide_tiles + low, high - low)],
                target.at[
                    pl.ds(low, high - low),
                    subs((peer if receiving else me_dn) * 2 * piece + c * piece, piece),
                    :,
                ],
                send.at[2 * slot + c, k],
                recv.at[2 * slot + c, peer if receiving else me_dn],
                "dn", peer,
            )
            for k, peer in enumerate(peers("dn"))
        ]

    halves = ((0, half_tiles), (half_tiles, wide_tiles))

    def up_in(source, target, send, recv, h, receiving):
        return [
            remote(
                source.at[:, subs(h * half + peer * piece, piece), :],
                target.at[h, pl.ds((peer if receiving else me_up) * tall_tiles, tall_tiles)],
                send.at[h, k], recv.at[h, peer if receiving else me_up], "up", peer,
            )
            for k, peer in enumerate(peers("up"))
        ]

    def up_out(source, target, send, recv, h, receiving):
        return [
            remote(
                source.at[h, pl.ds(peer * tall_tiles, tall_tiles)],
                target.at[:, subs(h * half + (peer if receiving else me_up) * piece, piece), :],
                send.at[h, k], recv.at[h, peer if receiving else me_up], "up", peer,
            )
            for k, peer in enumerate(peers("up"))
        ]

    def hop():
        def one(i, carry):
            picked = [x[columns[i * tile_k + k]] for k in range(tile_k)]
            result = jnp.dot(
                jnp.concatenate(picked, axis=1), w[i], preferred_element_type=jnp.float32
            )
            y[i] = result.astype(jnp.bfloat16)
            return carry

        lax.fori_loop(0, count, one, 0, unroll=2)

    def run(copies):
        for copy in copies:
            copy.start()
        finish(copies)

    def finish(copies):
        for copy in copies:
            copy.wait()

    def load_rows(c):
        for k, peer in enumerate(peers("dn") + [me_dn]):
            start = me_dn * 2 * piece + c * piece

            def one(t, carry):
                at = lanes(t * tile, tile)
                wide = lanes((peer * wide_tiles + t) * tile, tile)
                source = v.at[subs(start, piece), at] if k == n_dn - 1 else x1.at[c, :, wide]
                pltpu.make_async_copy(source, x.at[peer * wide_tiles + t], local.at[k]).start()
                return carry

            lax.fori_loop(0, wide_tiles, one, 0)
        for k, peer in enumerate(peers("dn") + [me_dn]):
            block = x.at[pl.ds(peer * wide_tiles, wide_tiles)]
            pltpu.make_async_copy(block, block, local.at[k]).wait()

    def load_columns(target, source, h):
        copies = []
        for k, peer in enumerate(peers("up")):
            at = pl.ds(peer * tall_tiles, tall_tiles)
            copies.append(pltpu.make_async_copy(target.at[h, at], x.at[at], local.at[k]))
        copies.append(
            pltpu.make_async_copy(
                source.at[:, subs(h * half + me_up * piece, piece), :],
                x.at[pl.ds(me_up * tall_tiles, tall_tiles)],
                local.at[n_up - 1],
            )
        )
        run(copies)

    def keep_rows(target, own_target, c):
        copies = [
            pltpu.make_async_copy(y, target.at[c], local.at[0]),
            pltpu.make_async_copy(
                y.at[pl.ds(me_dn * wide_tiles, wide_tiles)],
                own_target.at[:, subs(me_dn * 2 * piece + c * piece, piece), :],
                local.at[1],
            ),
        ]
        for copy in copies:
            copy.start()
        return copies

    def keep_columns(target, own_target, h):
        copies = [
            pltpu.make_async_copy(y, target.at[h], local.at[0]),
            pltpu.make_async_copy(
                y.at[pl.ds(me_up * tall_tiles, tall_tiles)],
                own_target.at[:, subs(h * half + me_up * piece, piece), :],
                local.at[1],
            ),
        ]
        for copy in copies:
            copy.start()
        return copies

    def turn(target, h, each):
        def one(i, carry):
            strip = a[i]
            flipped = strip.T
            for j in range(tall_tiles):
                b[j, subs(i * tile, tile), :] = flipped[:, j * tile : (j + 1) * tile]
            return each(i, strip, carry)

        carry = lax.fori_loop(0, half_tiles, one, each(None, None, None))
        run([pltpu.make_async_copy(b, target.at[:, subs(h * half, half), :], local.at[0])])
        return carry

    for c in range(2):
        launch(z_in(c, False))

    def moments(h):
        def each(i, strip, carry):
            if i is None:
                return (jnp.zeros((8, tile), jnp.float32), jnp.zeros((8, tile), jnp.float32))
            diagonal = jnp.dot(
                rows_t[...], occ_mine[:, lanes(h * half + i * tile, tile)],
                preferred_element_type=jnp.float32,
            )
            value = strip.astype(jnp.float32)
            square = value * value
            return (carry[0] + fold(diagonal * square), carry[1] + fold(square))

        return each

    def nothing(i, strip, carry):
        return 0

    sums = []
    for h in range(2):

        def fetch(i, carry):
            pltpu.make_async_copy(
                v.at[:, lanes(h * half + i * tile, tile)], a.at[i], local.at[0]
            ).start()
            return carry

        lax.fori_loop(0, half_tiles, fetch, 0)
        pltpu.make_async_copy(a, a, local.at[0]).wait()
        sums.append(turn(vt, h, moments(h)))
        launch(up_in(vt, x2, p_send, p_recv, h, False))
    weighted = jnp.sum(sums[0][0] + sums[1][0], axis=0, keepdims=True)
    norm = jnp.sum(sums[0][1] + sums[1][1], axis=0, keepdims=True)
    row = lax.broadcasted_iota(jnp.int32, (8, tile), 0)
    first[...] = jnp.where(row == 0, weighted, jnp.where(row == 1, norm, 0.0))

    def stage(g, slot):
        return pltpu.make_async_copy(
            tiles.at[pl.ds(g * group, group)], staged.at[slot], stage_sem.at[slot]
        )

    stage(0, 0).start()

    def prepare(g, carry):
        slot = lax.rem(g, 2)

        @pl.when(g + 1 < count // group)
        def _():
            stage(g + 1, 1 - slot).start()

        stage(g, slot).wait()

        def one(t, inner):
            for k in range(tile_k):
                i = g * group + t
                sign = (1 - 2 * signs[i * tile_k + k]).astype(jnp.float32)
                value = staged[slot, t, k].astype(jnp.float32) * sign
                w[i, k * tile : (k + 1) * tile, :] = value.astype(jnp.bfloat16).T
            return inner

        return lax.fori_loop(0, group, one, carry)

    lax.fori_loop(0, count // group, prepare, 0)

    totals = reduce_all(n_up, n_dn, me_up, me_dn, first, z_first, up_first, first_sems)
    sigma = coupling * jnp.sum(totals[0:1, :]) / jnp.maximum(jnp.sum(totals[1:2, :]), 1e-30)
    sigma_out[...] = jnp.full((8, tile), sigma, jnp.float32)

    def shifted(left, store):
        def one(j, carry):
            diagonal = coupling * jnp.dot(
                left, occ_all[:, lanes(j * tile, tile)], preferred_element_type=jnp.float32
            )
            value = y[j].astype(jnp.float32) + (diagonal - sigma) * x[j].astype(jnp.float32)
            store[j] = value.astype(jnp.bfloat16)
            return carry

        lax.fori_loop(0, count, one, 0, unroll=2)

    for h in range(2):
        arrive(up_in(vt, x2, p_send, p_recv, h, True))
        load_columns(x2, vt, h)
        hop()
        finish(keep_columns(u2, u0, h))
        launch(up_out(u2, u0, q_send, q_recv, h, False))
        shifted(cols_t[subs(h * half + me_up * piece, piece), :], y)
        run([pltpu.make_async_copy(y, g2.at[h], local.at[0])])

    for c in range(2):
        arrive(z_in(c, True))
        load_rows(c)
        hop()
        finish(keep_rows(dn1, d0, c))
        if c == 0:
            launch(z_out(dn1, d0, b_send, b_recv, halves[0], 0, 0, False))
        else:
            launch(z_out(dn1, d0, b_send, b_recv, halves[0], 0, 1, False))
            launch(z_out(dn1, d0, b_send, b_recv, halves[1], 1, 0, False))
            launch(z_out(dn1, d0, b_send, b_recv, halves[1], 1, 1, False))
        shifted(rows_t[subs(me_dn * 2 * piece + c * piece, piece), :], x)
        hop()
        finish(keep_rows(s1, s0, c))

    def flip(h):
        for c in range(2):
            arrive(z_out(dn1, d0, b_send, b_recv, halves[h], h, c, True))
        run([pltpu.make_async_copy(d0.at[pl.ds(h * half_tiles, half_tiles)], a, local.at[0])])
        turn(dt, h, nothing)
        launch(up_in(dt, d2, t_send, t_recv, h, False))

    def second(h):
        arrive(up_in(dt, d2, t_send, t_recv, h, True))
        load_columns(d2, dt, h)
        run([pltpu.make_async_copy(g2.at[h], y, local.at[0])])

        def one(j, carry):
            value = y[j].astype(jnp.float32) + 2.0 * x[j].astype(jnp.float32)
            x[j] = value.astype(jnp.bfloat16)
            return carry

        lax.fori_loop(0, count, one, 0, unroll=2)
        hop()
        finish(keep_columns(r2, r0, h))
        launch(up_out(r2, r0, o_send, o_recv, h, False))

    flip(0)
    for slot, span in enumerate(spans):
        for c in range(2):
            launch(z_out(s1, s0, c_send, c_recv, span, slot, c, False))
    second(0)
    flip(1)
    second(1)

    def strip_in(i, slot):
        at = subs(i * tile, tile)
        return [
            pltpu.make_async_copy(v.at[:, lanes(i * tile, tile)], flat.at[slot, 0], strip_sem.at[slot, 0]),
            pltpu.make_async_copy(d0.at[i], flat.at[slot, 1], strip_sem.at[slot, 1]),
            pltpu.make_async_copy(s0.at[i], flat.at[slot, 2], strip_sem.at[slot, 2]),
            pltpu.make_async_copy(u0.at[:, at, :], turned.at[slot, 0], strip_sem.at[slot, 3]),
            pltpu.make_async_copy(r0.at[:, at, :], turned.at[slot, 1], strip_sem.at[slot, 4]),
        ]

    def strip_out(i, slot):
        return [
            pltpu.make_async_copy(made.at[slot, 0], m_out.at[i], made_sem.at[slot, 0]),
            pltpu.make_async_copy(made.at[slot, 1], w_out.at[i], made_sem.at[slot, 1]),
        ]

    def combine(low, high, carry):
        for copy in strip_in(low, 0):
            copy.start()

        def one(i, carry):
            slot = lax.rem(i - low, 2)

            @pl.when(i + 1 < high)
            def _():
                for copy in strip_in(i + 1, 1 - slot):
                    copy.start()

            finish(strip_in(i, slot))

            @pl.when(i - low >= 2)
            def _():
                finish(strip_out(i - 2, slot))

            def block(j, carry):
                at = subs(j * tile, tile)
                value = flat[slot, 0, at, :].astype(jnp.float32)
                diagonal = coupling * jnp.dot(
                    rows_t[at, :], occ_mine[:, lanes(i * tile, tile)],
                    preferred_element_type=jnp.float32,
                )
                shift = diagonal - sigma
                total = flat[slot, 1, at, :].astype(jnp.float32)
                total = total + turned[slot, 0, j].T.astype(jnp.float32) + shift * value
                m = flat[slot, 2, at, :].astype(jnp.float32)
                m = m + turned[slot, 1, j].T.astype(jnp.float32) + shift * total
                made[slot, 0, at, :] = m.astype(jnp.bfloat16)
                made[slot, 1, at, :] = total.astype(jnp.bfloat16)
                pairs = (m * m, m * total, m * value, total * total, total * value, value * value)
                return tuple(c + fold(p) for c, p in zip(carry, pairs))

            carry = lax.fori_loop(0, tall_tiles, block, carry)
            for copy in strip_out(i, slot):
                copy.start()
            return carry

        carry = lax.fori_loop(low, high, one, carry)
        for i in range(max(low, high - 2), high):
            finish(strip_out(i, (i - low) % 2))
        return carry

    carry = tuple(jnp.zeros((8, tile), jnp.float32) for _ in range(6))
    for h in range(2):
        arrive(up_out(u2, u0, q_send, q_recv, h, True))
        arrive(up_out(r2, r0, o_send, o_recv, h, True))
    for slot, span in enumerate(spans):
        for c in range(2):
            arrive(z_out(s1, s0, c_send, c_recv, span, slot, c, True))
        carry = combine(span[0], span[1], carry)
    packed = jnp.zeros((8, tile), jnp.float32)
    for k in range(6):
        packed = jnp.where(row == k, jnp.sum(carry[k], axis=0, keepdims=True), packed)
    last[...] = packed
    gram_out[...] = reduce_all(n_up, n_dn, me_up, me_dn, last, z_last, up_last, last_sems)
    for copy in started:
        copy.wait_send()


def exchange(v, tiles, columns, signs, occ_all, occ_mine, rows_t, cols_t):
    n_up = lax.axis_size("up")
    n_dn = lax.axis_size("dn")
    count, tile_k, tile, _ = tiles.shape
    rows, cols = v.shape
    piece = rows // n_dn // 2
    group = max(d for d in range(1, 9) if count % d == 0)
    wide, tall = cols // tile, rows // tile
    cuts = sorted({0, wide // 2, wide - wide // 4, wide - wide // 12, wide})
    spans = tuple(zip(cuts[:-1], cuts[1:]))
    bf16, f32 = jnp.bfloat16, jnp.float32
    natural = jax.ShapeDtypeStruct((wide, rows, tile), bf16)
    turned = jax.ShapeDtypeStruct((tall, cols, tile), bf16)
    strips = jax.ShapeDtypeStruct((2, count, piece, tile), bf16)
    landed = jax.ShapeDtypeStruct((2, piece, count * tile), bf16)
    small = jax.ShapeDtypeStruct((8, tile), f32)
    dma = pltpu.SemaphoreType.DMA
    z4 = [dma((4, n_dn - 1)), dma((4, n_dn))]
    zs = [dma((2 * len(spans), n_dn - 1)), dma((2 * len(spans), n_dn))]
    up2 = [dma((2, n_up - 1)), dma((2, n_up))]
    sums = [dma((n_dn - 1,)), dma((n_dn,)), dma((n_up - 1,)), dma((n_up,))]
    any_spec = pl.BlockSpec(memory_space=ANY)
    vmem = pl.BlockSpec(memory_space=pltpu.VMEM)
    smem = pl.BlockSpec(memory_space=pltpu.SMEM)
    outs = pl.pallas_call(
        functools.partial(kernel, (n_up, n_dn, count, tile_k, tile, group, spans)),
        in_specs=[smem, smem, any_spec, any_spec, vmem, vmem, vmem, vmem],
        out_specs=[any_spec] * 2 + [vmem] * 2 + [any_spec] * 14,
        out_shape=[natural, natural, small, small, natural, natural, turned, turned, landed]
        + [strips] * 6 + [turned, turned, strips],
        scratch_shapes=[
            pltpu.VMEM((count, piece, tile), bf16),
            pltpu.VMEM((count, piece, tile), bf16),
            pltpu.VMEM((count, tile_k * tile, tile), bf16),
            pltpu.VMEM((wide // 2, rows, tile), bf16),
            pltpu.VMEM((tall, cols // 2, tile), bf16),
            pltpu.VMEM((2, group, tile_k, tile, tile), bf16),
            pltpu.VMEM((2, 3, rows, tile), bf16),
            pltpu.VMEM((2, 2, tall, tile, tile), bf16),
            pltpu.VMEM((2, 2, rows, tile), bf16),
            pltpu.VMEM((8, tile), f32),
            pltpu.VMEM((8, tile), f32),
            pltpu.VMEM((n_dn, 8, tile), f32),
            pltpu.VMEM((n_up, 8, tile), f32),
            pltpu.VMEM((n_dn, 8, tile), f32),
            pltpu.VMEM((n_up, 8, tile), f32),
            dma((max(n_up, n_dn),)),
            dma((2,)),
            dma((2, 5)),
            dma((2, 2)),
            dma((2, n_dn - 1)), dma((2, n_dn)),
            *z4, *zs, *up2, *up2, *up2, *up2, sums, sums,
        ],
        compiler_params=pltpu.CompilerParams(
            collective_id=0, has_side_effects=True, vmem_limit_bytes=60 * 1024 * 1024
        ),
        cost_estimate=pl.CostEstimate(
            flops=8 * rows * cols * tile_k * tile, bytes_accessed=60 * rows * cols, transcendentals=0
        ),
    )(columns, signs, v, tiles, occ_all, occ_mine, rows_t, cols_t)
    return outs[:4]


def final_kernel(m, w, v, sigma, gram, out, scalars):
    mm, mw, mv, ww, wv, vv = (jnp.sum(gram[k : k + 1, :], axis=1, keepdims=True) for k in range(6))
    shift = sigma[0:1, 0:1]
    scale = 1.0 / jnp.maximum(jnp.sqrt(vv), 1.0)
    square = scale * scale
    alpha1 = square * (wv + shift * vv)
    delta = alpha1 - shift
    norm = ww - 2.0 * delta * wv + delta * delta * vv
    beta1 = jnp.sqrt(jnp.maximum(square * norm, 1.0))
    gain = square / (beta1 * beta1)
    length = gain * norm
    offset = mw - delta * mv - delta * (ww - delta * wv) - beta1 * beta1 * (wv - delta * vv)
    offset = gain * offset
    alpha2 = offset + shift * length
    c1 = -(delta + offset + shift * (length - 1.0))
    c2 = (alpha2 - shift) * delta - beta1 * beta1
    residual = mm + c1 * c1 * ww + c2 * c2 * vv + 2.0 * (c1 * mw + c2 * mv + c1 * c2 * wv)
    beta2 = jnp.sqrt(jnp.maximum(gain * residual, 1.0))
    factor = scale / (beta1 * beta2)
    value = m[0].astype(jnp.float32) + c1 * w[0].astype(jnp.float32) + c2 * v[...].astype(jnp.float32)
    out[...] = (factor * value).astype(jnp.bfloat16)
    row = lax.broadcasted_iota(jnp.int32, scalars.shape, 0)
    found = jnp.zeros(scalars.shape, jnp.float32)
    for k, value in enumerate((alpha1, alpha2, beta1, beta2)):
        found = jnp.where(row == k, value, found)
    scalars[...] = found


def finish_all(m, w, v, sigma, gram):
    rows, cols = v.shape
    tile = m.shape[2]
    column = pl.BlockSpec((rows, tile), lambda i: (0, i))
    strip = pl.BlockSpec((1, rows, tile), lambda i: (i, 0, 0))
    small = pl.BlockSpec((8, tile), lambda i: (0, 0))
    return pl.pallas_call(
        final_kernel,
        grid=(cols // tile,),
        in_specs=[strip, strip, column, small, small],
        out_specs=[column, small],
        out_shape=[
            jax.ShapeDtypeStruct((rows, cols), jnp.bfloat16),
            jax.ShapeDtypeStruct((8, tile), jnp.float32),
        ],
    )(m, w, v, sigma, gram)


def fused_body(start_vector, hop_tiles, tile_columns, tile_signs, occupation):
    rows, cols = start_vector.shape
    row_start = lax.axis_index("up") * rows
    col_start = lax.axis_index("dn") * cols
    occ = occupation.astype(jnp.bfloat16)
    occ_mine = lax.dynamic_slice_in_dim(occ, col_start, cols, 1)
    rows_t = lax.dynamic_slice_in_dim(occ, row_start, rows, 1).T
    cols_t = occ_mine.T
    m, w, sigma, gram = exchange(
        start_vector, hop_tiles, tile_columns.reshape(-1), tile_signs.reshape(-1),
        occ, occ_mine, rows_t, cols_t,
    )
    final, scalars = finish_all(m, w, start_vector, sigma, gram)
    return (final, scalars[0:2, 0], scalars[2:4, 0])


def fits(n_up, n_dn, rows, cols, tile):
    even = rows % (16 * n_dn) == 0 and cols % (16 * n_up) == 0
    return even and rows % tile == 0 and cols % (2 * tile) == 0


def chosen_body(start_vector, hop_tiles, *rest):
    rows, cols = start_vector.shape
    good = fits(lax.axis_size("up"), lax.axis_size("dn"), rows, cols, hop_tiles.shape[2])
    return (fused_body if good else body)(start_vector, hop_tiles, *rest)


def solution(mesh):
    placed = (P("up", "dn"), P(), P(), P(), P())
    return jax.shard_map(
        chosen_body, mesh=mesh, in_specs=placed, out_specs=(P("up", "dn"), P(), P()), check_vma=False
    )
```

```python
import functools

import jax
import jax.numpy as jnp
from jax import lax
from jax.experimental import pallas as pl
from jax.experimental.pallas import tpu as pltpu
from jax.sharding import PartitionSpec as P

STEPS = 2


coupling = 4.0


def hop_kernel(tile_k, tile, group, parts_tiles, columns_ref, x_ref, tiles_ref, out_ref):
    first = pl.program_id(0) * group

    def one_tile(t, carry):
        picked = []
        for k in range(tile_k):
            column = columns_ref[(first + t) * tile_k + k]
            at = pl.multiple_of(lax.rem(column, parts_tiles) * tile, tile)
            picked.append(x_ref[lax.div(column, parts_tiles), :, pl.ds(at, tile)])
        left = jnp.concatenate(picked, axis=1)
        result = jnp.dot(left, tiles_ref[t], preferred_element_type=jnp.float32)
        out_ref[0, :, pl.ds(pl.multiple_of(t * tile, tile), tile)] = result.astype(jnp.bfloat16)
        return carry

    lax.fori_loop(0, group, one_tile, 0)


def hop_blocks(x, stacked, columns, tile_k):
    parts, rows, width = x.shape
    tiles, depth, tile = stacked.shape
    if width % tile:
        joined = x.transpose(1, 0, 2).reshape(1, rows, parts * width)
        hopped = hop_blocks(joined, stacked, columns, tile_k)
        return hopped.reshape(rows, parts, width).transpose(1, 0, 2)
    parts_tiles = width // tile
    group = max(d for d in range(1, 17) if parts_tiles % d == 0)
    per_part = parts_tiles // group
    return pl.pallas_call(
        functools.partial(hop_kernel, tile_k, tile, group, parts_tiles),
        grid_spec=pltpu.PrefetchScalarGridSpec(
            num_scalar_prefetch=1,
            grid=(tiles // group,),
            in_specs=[
                pl.BlockSpec((parts, rows, width), lambda i, c: (0, 0, 0)),
                pl.BlockSpec((group, depth, tile), lambda i, c: (i, 0, 0)),
            ],
            out_specs=pl.BlockSpec(
                (1, rows, group * tile), lambda i, c: (i // per_part, 0, i % per_part)
            ),
        ),
        out_shape=jax.ShapeDtypeStruct(x.shape, jnp.bfloat16),
        compiler_params=pltpu.CompilerParams(vmem_limit_bytes=56 * 1024 * 1024),
        cost_estimate=pl.CostEstimate(
            flops=2 * rows * tiles * depth * tile,
            bytes_accessed=4 * rows * parts * width + 2 * tiles * depth * tile,
            transcendentals=0,
        ),
    )(columns, x, stacked)


def body(start_vector, hop_tiles, tile_columns, tile_signs, occupation):
    tiles, tile_k, tile, _ = hop_tiles.shape
    signed = hop_tiles * (1 - 2 * tile_signs).astype(jnp.bfloat16)[:, :, None, None]
    stacked = signed.transpose(0, 1, 3, 2).reshape(tiles, tile_k * tile, tile)
    columns = tile_columns.reshape(-1)
    block_rows, block_cols = start_vector.shape
    count_up = lax.axis_size("up")
    count_down = lax.axis_size("dn")
    row_start = lax.axis_index("up") * block_rows
    col_start = lax.axis_index("dn") * block_cols
    occ_rows = lax.dynamic_slice_in_dim(occupation, row_start, block_rows, 1).astype(jnp.bfloat16)
    occ_cols = lax.dynamic_slice_in_dim(occupation, col_start, block_cols, 1).astype(jnp.bfloat16)
    diagonal = (
        coupling * jnp.einsum("sa,sb->ab", occ_rows, occ_cols, preferred_element_type=jnp.float32)
    ).astype(jnp.bfloat16)
    total = lax.psum(jnp.sum(jnp.square(start_vector.astype(jnp.float32))), ("up", "dn"))
    scale = 1.0 / jnp.maximum(jnp.sqrt(total), 1.0)
    vector = start_vector.astype(jnp.float32) * scale
    length = total / jnp.maximum(total, 1.0)
    previous = None
    beta_value = None
    alpha_list = []
    beta_list = []
    for iteration in range(STEPS):
        rounded = start_vector if iteration == 0 else vector.astype(jnp.bfloat16)
        down = rounded.reshape(count_down, block_rows // count_down, block_cols)
        up = rounded.T.reshape(count_up, block_cols // count_up, block_rows)
        down = lax.all_to_all(down, "dn", 0, 0, tiled=True)
        up = lax.all_to_all(up, "up", 0, 0, tiled=True)
        down = hop_blocks(down, stacked, columns, tile_k)
        down = lax.all_to_all(down, "dn", 0, 0, tiled=True)
        up = hop_blocks(up, stacked, columns, tile_k)
        up = lax.all_to_all(up, "up", 0, 0, tiled=True)
        hopped_down = down.reshape(block_rows, block_cols)
        hopped_up = up.reshape(block_cols, block_rows).T
        hopped = hopped_up.astype(jnp.float32) + hopped_down.astype(jnp.float32)
        if iteration == 0:
            work = hopped * scale + diagonal * vector
        else:
            work = hopped + diagonal * vector - beta_value * previous
        intersect, square = lax.psum((jnp.sum(work * vector), jnp.sum(work * work)), ("up", "dn"))
        work = work - intersect * vector
        residual = square - 2.0 * intersect * intersect + intersect * intersect * length
        beta_value = jnp.sqrt(jnp.maximum(residual, 1.0))
        length = residual / jnp.maximum(residual, 1.0)
        previous = vector
        vector = work / beta_value
        alpha_list.append(intersect)
        beta_list.append(beta_value)
    final = vector.astype(jnp.bfloat16)
    return (final, jnp.stack(alpha_list), jnp.stack(beta_list))


MESH = pl.DeviceIdType.MESH
ANY = pl.ANY


def remote(src, dst, send_sem, recv_sem, axis, peer):
    return pltpu.make_async_remote_copy(
        src_ref=src,
        dst_ref=dst,
        send_sem=send_sem,
        recv_sem=recv_sem,
        device_id={axis: peer},
        device_id_type=MESH,
    )


def reduce_all(n_up, n_dn, me_up, me_dn, mine, z_slots, up_slots, sems):
    z_send, z_recv, up_send, up_recv = sems
    z_slots[me_dn] = mine[...]
    copies = []
    for d in range(1, n_dn):
        peer = lax.rem(me_dn + d, n_dn)
        copy = remote(mine, z_slots.at[me_dn], z_send.at[d - 1], z_recv.at[me_dn], "dn", peer)
        copy.start()
        copies.append(copy)
    for d in range(1, n_dn):
        peer = lax.rem(me_dn + d, n_dn)
        remote(mine, z_slots.at[peer], z_send.at[d - 1], z_recv.at[peer], "dn", peer).wait_recv()
    for copy in copies:
        copy.wait_send()
    mine[...] = jnp.sum(z_slots[...], axis=0)
    up_slots[me_up] = mine[...]
    copies = []
    for d in range(1, n_up):
        peer = lax.rem(me_up + d, n_up)
        copy = remote(mine, up_slots.at[me_up], up_send.at[d - 1], up_recv.at[me_up], "up", peer)
        copy.start()
        copies.append(copy)
    for d in range(1, n_up):
        peer = lax.rem(me_up + d, n_up)
        remote(mine, up_slots.at[peer], up_send.at[d - 1], up_recv.at[peer], "up", peer).wait_recv()
    for copy in copies:
        copy.wait_send()
    return jnp.sum(up_slots[...], axis=0)


def fold(x):
    return jnp.sum(x.reshape(-1, 8, x.shape[-1]), axis=0)


def kernel(
    dims, columns, signs, v, tiles, occ_all, occ_mine, rows_t, cols_t,
    m_out, w_out, sigma_out, gram_out,
    d0, s0, u0, r0, x1, x2, dn1, s1, u2, g2, d2, vt, dt, r2,
    x, y, w, a, b, staged, flat, turned, made, last, z_last, up_last,
    local, stage_sem, strip_sem, made_sem, a_send, a_recv, b_send, b_recv, c_send, c_recv,
    p_send, p_recv, q_send, q_recv, t_send, t_recv, o_send, o_recv, last_sems,
):
    n_up, n_dn, count, tile_k, tile, group, spans = dims
    rows, cols = v.shape
    half = cols // 2
    wide_tiles = cols // tile
    tall_tiles = rows // tile
    half_tiles = wide_tiles // 2
    wide = occ_all.shape[1]
    piece = x.shape[1]
    me_up = lax.axis_index("up")
    me_dn = lax.axis_index("dn")

    barrier = pltpu.get_barrier_semaphore()
    for d in range(1, n_dn):
        pl.semaphore_signal(
            barrier, inc=1, device_id={"dn": lax.rem(me_dn + d, n_dn)}, device_id_type=MESH
        )
    for d in range(1, n_up):
        pl.semaphore_signal(
            barrier, inc=1, device_id={"up": lax.rem(me_up + d, n_up)}, device_id_type=MESH
        )
    pl.semaphore_wait(barrier, n_dn + n_up - 2)

    def lanes(start, size):
        return pl.ds(pl.multiple_of(start, tile), size)

    def subs(start, size):
        return pl.ds(pl.multiple_of(start, 8), size)

    def peers(axis):
        n, me = (n_dn, me_dn) if axis == "dn" else (n_up, me_up)
        return [lax.rem(me + d, n) for d in range(1, n)]

    started = []

    def launch(copies):
        for copy in copies:
            copy.start()
        started.extend(copies)

    def arrive(name, copies):
        with jax.named_scope(name):
            for copy in copies:
                copy.wait_recv()

    def z_in(c, receiving):
        return [
            remote(
                v.at[subs(peer * 2 * piece + c * piece, piece), :],
                x1.at[c, :, lanes((peer if receiving else me_dn) * cols, cols)],
                a_send.at[c, k], a_recv.at[c, peer if receiving else me_dn], "dn", peer,
            )
            for k, peer in enumerate(peers("dn"))
        ]

    def z_out(source, target, send, recv, span, slot, c, receiving):
        low, high = span
        return [
            remote(
                source.at[c, pl.ds(peer * wide_tiles + low, high - low)],
                target.at[
                    pl.ds(low, high - low),
                    subs((peer if receiving else me_dn) * 2 * piece + c * piece, piece),
                    :,
                ],
                send.at[2 * slot + c, k],
                recv.at[2 * slot + c, peer if receiving else me_dn],
                "dn", peer,
            )
            for k, peer in enumerate(peers("dn"))
        ]

    halves = ((0, half_tiles), (half_tiles, wide_tiles))

    def up_in(source, target, send, recv, h, receiving):
        return [
            remote(
                source.at[:, subs(h * half + peer * piece, piece), :],
                target.at[h, pl.ds((peer if receiving else me_up) * tall_tiles, tall_tiles)],
                send.at[h, k], recv.at[h, peer if receiving else me_up], "up", peer,
            )
            for k, peer in enumerate(peers("up"))
        ]

    def up_out(source, target, send, recv, h, receiving):
        return [
            remote(
                source.at[h, pl.ds(peer * tall_tiles, tall_tiles)],
                target.at[:, subs(h * half + (peer if receiving else me_up) * piece, piece), :],
                send.at[h, k], recv.at[h, peer if receiving else me_up], "up", peer,
            )
            for k, peer in enumerate(peers("up"))
        ]

    def hop():
        def one(i, carry):
            picked = [x[columns[i * tile_k + k]] for k in range(tile_k)]
            result = jnp.dot(
                jnp.concatenate(picked, axis=1), w[i], preferred_element_type=jnp.float32
            )
            y[i] = result.astype(jnp.bfloat16)
            return carry

        with jax.named_scope("hop"):
            lax.fori_loop(0, count, one, 0, unroll=8)

    def run(copies):
        for copy in copies:
            copy.start()
        finish(copies)

    def finish(copies):
        for copy in copies:
            copy.wait()

    def load_rows(c):
        for k, peer in enumerate(peers("dn") + [me_dn]):
            start = me_dn * 2 * piece + c * piece

            def one(t, carry):
                at = lanes(t * tile, tile)
                wide = lanes((peer * wide_tiles + t) * tile, tile)
                source = v.at[subs(start, piece), at] if k == n_dn - 1 else x1.at[c, :, wide]
                pltpu.make_async_copy(source, x.at[peer * wide_tiles + t], local.at[k]).start()
                return carry

            lax.fori_loop(0, wide_tiles, one, 0)
        for k, peer in enumerate(peers("dn") + [me_dn]):
            block = x.at[pl.ds(peer * wide_tiles, wide_tiles)]
            pltpu.make_async_copy(block, block, local.at[k]).wait()

    def load_columns(target, source, h):
        copies = []
        for k, peer in enumerate(peers("up")):
            at = pl.ds(peer * tall_tiles, tall_tiles)
            copies.append(pltpu.make_async_copy(target.at[h, at], x.at[at], local.at[k]))
        copies.append(
            pltpu.make_async_copy(
                source.at[:, subs(h * half + me_up * piece, piece), :],
                x.at[pl.ds(me_up * tall_tiles, tall_tiles)],
                local.at[n_up - 1],
            )
        )
        run(copies)

    def keep_rows(target, own_target, c):
        copies = [
            pltpu.make_async_copy(y, target.at[c], local.at[0]),
            pltpu.make_async_copy(
                y.at[pl.ds(me_dn * wide_tiles, wide_tiles)],
                own_target.at[:, subs(me_dn * 2 * piece + c * piece, piece), :],
                local.at[1],
            ),
        ]
        for copy in copies:
            copy.start()
        return copies

    def keep_columns(target, own_target, h):
        copies = [
            pltpu.make_async_copy(y, target.at[h], local.at[0]),
            pltpu.make_async_copy(
                y.at[pl.ds(me_up * tall_tiles, tall_tiles)],
                own_target.at[:, subs(h * half + me_up * piece, piece), :],
                local.at[1],
            ),
        ]
        for copy in copies:
            copy.start()
        return copies

    def turn(target, h):
        def one(i, carry):
            flipped = a[i].T
            for j in range(tall_tiles):
                b[j, subs(i * tile, tile), :] = flipped[:, j * tile : (j + 1) * tile]
            return carry

        lax.fori_loop(0, half_tiles, one, 0)
        run([pltpu.make_async_copy(b, target.at[:, subs(h * half, half), :], local.at[0])])

    for c in range(2):
        launch(z_in(c, False))

    for h in range(2):

        def fetch(i, carry):
            pltpu.make_async_copy(
                v.at[:, lanes(h * half + i * tile, tile)], a.at[i], local.at[0]
            ).start()
            return carry

        lax.fori_loop(0, half_tiles, fetch, 0)
        pltpu.make_async_copy(a, a, local.at[0]).wait()
        turn(vt, h)
        launch(up_in(vt, x2, p_send, p_recv, h, False))
    def stage(g, slot):
        return pltpu.make_async_copy(
            tiles.at[pl.ds(g * group, group)], staged.at[slot], stage_sem.at[slot]
        )

    stage(0, 0).start()

    def prepare(g, carry):
        slot = lax.rem(g, 2)

        @pl.when(g + 1 < count // group)
        def _():
            stage(g + 1, 1 - slot).start()

        stage(g, slot).wait()

        def one(t, inner):
            for k in range(tile_k):
                i = g * group + t
                sign = (1 - 2 * signs[i * tile_k + k]).astype(jnp.float32)
                value = staged[slot, t, k].astype(jnp.float32) * sign
                w[i, k * tile : (k + 1) * tile, :] = value.astype(jnp.bfloat16).T
            return inner

        return lax.fori_loop(0, group, one, carry)

    with jax.named_scope("prepare"):
        lax.fori_loop(0, count // group, prepare, 0)

    filled = jnp.sum(occ_all[...].astype(jnp.float32), axis=1, keepdims=True) / wide
    sigma = coupling * jnp.sum(filled * filled)
    sigma_out[...] = jnp.full((8, tile), sigma, jnp.float32)

    def shifted(left, store):
        def one(j, carry):
            diagonal = coupling * jnp.dot(
                left, occ_all[:, lanes(j * tile, tile)], preferred_element_type=jnp.float32
            )
            value = y[j].astype(jnp.float32) + (diagonal - sigma) * x[j].astype(jnp.float32)
            store[j] = value.astype(jnp.bfloat16)
            return carry

        lax.fori_loop(0, count, one, 0, unroll=2)

    for h in range(2):
        arrive(f"wait_x2_{h}", up_in(vt, x2, p_send, p_recv, h, True))
        load_columns(x2, vt, h)
        hop()
        finish(keep_columns(u2, u0, h))
        launch(up_out(u2, u0, q_send, q_recv, h, False))
        shifted(cols_t[subs(h * half + me_up * piece, piece), :], y)
        run([pltpu.make_async_copy(y, g2.at[h], local.at[0])])

    behind = []
    for c in range(2):
        arrive(f"wait_x1_{c}", z_in(c, True))
        load_rows(c)
        hop()
        finish(keep_rows(dn1, d0, c))
        if c == 0:
            launch(z_out(dn1, d0, b_send, b_recv, halves[0], 0, 0, False))
        else:
            launch(z_out(dn1, d0, b_send, b_recv, halves[0], 0, 1, False))
            for part in range(2):
                late = z_out(dn1, d0, b_send, b_recv, halves[1], 1, part, False)
                for copy in late:
                    copy.start()
                behind.extend(late)
        shifted(rows_t[subs(me_dn * 2 * piece + c * piece, piece), :], x)
        hop()
        finish(keep_rows(s1, s0, c))

    def flip(h):
        for c in range(2):
            arrive(f"wait_d0_{h}", z_out(dn1, d0, b_send, b_recv, halves[h], h, c, True))
        run([pltpu.make_async_copy(d0.at[pl.ds(h * half_tiles, half_tiles)], a, local.at[0])])
        turn(dt, h)
        launch(up_in(dt, d2, t_send, t_recv, h, False))

    def second(h):
        arrive(f"wait_d2_{h}", up_in(dt, d2, t_send, t_recv, h, True))
        load_columns(d2, dt, h)
        run([pltpu.make_async_copy(g2.at[h], y, local.at[0])])

        def one(j, carry):
            value = y[j].astype(jnp.float32) + 2.0 * x[j].astype(jnp.float32)
            x[j] = value.astype(jnp.bfloat16)
            return carry

        lax.fori_loop(0, count, one, 0, unroll=2)
        hop()
        finish(keep_columns(r2, r0, h))
        launch(up_out(r2, r0, o_send, o_recv, h, False))

    flip(0)
    second(0)
    with jax.named_scope("wait_behind"):
        for copy in behind:
            copy.wait_send()
    for slot, span in enumerate(spans):
        for c in range(2):
            launch(z_out(s1, s0, c_send, c_recv, span, slot, c, False))
    flip(1)
    second(1)

    def strip_in(i, slot):
        at = subs(i * tile, tile)
        return [
            pltpu.make_async_copy(v.at[:, lanes(i * tile, tile)], flat.at[slot, 0], strip_sem.at[slot, 0]),
            pltpu.make_async_copy(d0.at[i], flat.at[slot, 1], strip_sem.at[slot, 1]),
            pltpu.make_async_copy(s0.at[i], flat.at[slot, 2], strip_sem.at[slot, 2]),
            pltpu.make_async_copy(u0.at[:, at, :], turned.at[slot, 0], strip_sem.at[slot, 3]),
            pltpu.make_async_copy(r0.at[:, at, :], turned.at[slot, 1], strip_sem.at[slot, 4]),
        ]

    def strip_out(i, slot):
        return [
            pltpu.make_async_copy(made.at[slot, 0], m_out.at[i], made_sem.at[slot, 0]),
            pltpu.make_async_copy(made.at[slot, 1], w_out.at[i], made_sem.at[slot, 1]),
        ]

    def combine(low, high, carry):
        for copy in strip_in(low, 0):
            copy.start()

        def one(i, carry):
            slot = lax.rem(i - low, 2)

            @pl.when(i + 1 < high)
            def _():
                for copy in strip_in(i + 1, 1 - slot):
                    copy.start()

            finish(strip_in(i, slot))

            @pl.when(i - low >= 2)
            def _():
                finish(strip_out(i - 2, slot))

            def block(j, carry):
                at = subs(j * tile, tile)
                value = flat[slot, 0, at, :].astype(jnp.float32)
                diagonal = coupling * jnp.dot(
                    rows_t[at, :], occ_mine[:, lanes(i * tile, tile)],
                    preferred_element_type=jnp.float32,
                )
                shift = diagonal - sigma
                total = flat[slot, 1, at, :].astype(jnp.float32)
                total = total + turned[slot, 0, j].T.astype(jnp.float32) + shift * value
                m = flat[slot, 2, at, :].astype(jnp.float32)
                m = m + turned[slot, 1, j].T.astype(jnp.float32) + shift * total
                made[slot, 0, at, :] = m.astype(jnp.bfloat16)
                made[slot, 1, at, :] = total.astype(jnp.bfloat16)
                pairs = (m * m, m * total, m * value, total * total, total * value, value * value)
                return tuple(c + fold(p) for c, p in zip(carry, pairs))

            carry = lax.fori_loop(0, tall_tiles, block, carry, unroll=True)
            for copy in strip_out(i, slot):
                copy.start()
            return carry

        carry = lax.fori_loop(low, high, one, carry)
        for i in range(max(low, high - 2), high):
            finish(strip_out(i, (i - low) % 2))
        return carry

    carry = tuple(jnp.zeros((8, tile), jnp.float32) for _ in range(6))
    for slot, span in enumerate(spans):
        if span[0] in (0, half_tiles):
            arrive("wait_u0", up_out(u2, u0, q_send, q_recv, min(slot, 1), True))
            arrive("wait_r0", up_out(r2, r0, o_send, o_recv, min(slot, 1), True))
        for c in range(2):
            arrive(f"wait_s0_{slot}", z_out(s1, s0, c_send, c_recv, span, slot, c, True))
        with jax.named_scope(f"combine_{slot}"):
            carry = combine(span[0], span[1], carry)
    row = lax.broadcasted_iota(jnp.int32, (8, tile), 0)
    packed = jnp.zeros((8, tile), jnp.float32)
    for k in range(6):
        packed = jnp.where(row == k, jnp.sum(carry[k], axis=0, keepdims=True), packed)
    last[...] = packed
    with jax.named_scope("reduce_last"):
        gram_out[...] = reduce_all(n_up, n_dn, me_up, me_dn, last, z_last, up_last, last_sems)
    with jax.named_scope("drain"):
        for copy in started:
            copy.wait_send()


def exchange(v, tiles, columns, signs, occ_all, occ_mine, rows_t, cols_t):
    n_up = lax.axis_size("up")
    n_dn = lax.axis_size("dn")
    count, tile_k, tile, _ = tiles.shape
    rows, cols = v.shape
    piece = rows // n_dn // 2
    group = max(d for d in range(1, 9) if count % d == 0)
    wide, tall = cols // tile, rows // tile
    cuts = sorted({0, wide // 2, wide - wide // 4, wide - wide // 12, wide})
    spans = tuple(zip(cuts[:-1], cuts[1:]))
    bf16, f32 = jnp.bfloat16, jnp.float32
    natural = jax.ShapeDtypeStruct((wide, rows, tile), bf16)
    turned = jax.ShapeDtypeStruct((tall, cols, tile), bf16)
    strips = jax.ShapeDtypeStruct((2, count, piece, tile), bf16)
    landed = jax.ShapeDtypeStruct((2, piece, count * tile), bf16)
    small = jax.ShapeDtypeStruct((8, tile), f32)
    dma = pltpu.SemaphoreType.DMA
    z4 = [dma((4, n_dn - 1)), dma((4, n_dn))]
    zs = [dma((2 * len(spans), n_dn - 1)), dma((2 * len(spans), n_dn))]
    up2 = [dma((2, n_up - 1)), dma((2, n_up))]
    sums = [dma((n_dn - 1,)), dma((n_dn,)), dma((n_up - 1,)), dma((n_up,))]
    any_spec = pl.BlockSpec(memory_space=ANY)
    vmem = pl.BlockSpec(memory_space=pltpu.VMEM)
    smem = pl.BlockSpec(memory_space=pltpu.SMEM)
    outs = pl.pallas_call(
        functools.partial(kernel, (n_up, n_dn, count, tile_k, tile, group, spans)),
        in_specs=[smem, smem, any_spec, any_spec, vmem, vmem, vmem, vmem],
        out_specs=[any_spec] * 2 + [vmem] * 2 + [any_spec] * 14,
        out_shape=[natural, natural, small, small, natural, natural, turned, turned, landed]
        + [strips] * 6 + [turned, turned, strips],
        scratch_shapes=[
            pltpu.VMEM((count, piece, tile), bf16),
            pltpu.VMEM((count, piece, tile), bf16),
            pltpu.VMEM((count, tile_k * tile, tile), bf16),
            pltpu.VMEM((wide // 2, rows, tile), bf16),
            pltpu.VMEM((tall, cols // 2, tile), bf16),
            pltpu.VMEM((2, group, tile_k, tile, tile), bf16),
            pltpu.VMEM((2, 3, rows, tile), bf16),
            pltpu.VMEM((2, 2, tall, tile, tile), bf16),
            pltpu.VMEM((2, 2, rows, tile), bf16),
            pltpu.VMEM((8, tile), f32),
            pltpu.VMEM((n_dn, 8, tile), f32),
            pltpu.VMEM((n_up, 8, tile), f32),
            dma((max(n_up, n_dn),)),
            dma((2,)),
            dma((2, 5)),
            dma((2, 2)),
            dma((2, n_dn - 1)), dma((2, n_dn)),
            *z4, *zs, *up2, *up2, *up2, *up2, sums,
        ],
        compiler_params=pltpu.CompilerParams(
            collective_id=0, has_side_effects=True, vmem_limit_bytes=60 * 1024 * 1024
        ),
        cost_estimate=pl.CostEstimate(
            flops=8 * rows * cols * tile_k * tile, bytes_accessed=60 * rows * cols, transcendentals=0
        ),
    )(columns, signs, v, tiles, occ_all, occ_mine, rows_t, cols_t)
    return outs[:4]


def final_scalars(sigma, gram):
    mm, mw, mv, ww, wv, vv = (jnp.sum(gram[k : k + 1, :], axis=1, keepdims=True) for k in range(6))
    shift = sigma[0:1, 0:1]
    scale = 1.0 / jnp.maximum(jnp.sqrt(vv), 1.0)
    square = scale * scale
    alpha1 = square * (wv + shift * vv)
    delta = alpha1 - shift
    norm = ww - 2.0 * delta * wv + delta * delta * vv
    beta1 = jnp.sqrt(jnp.maximum(square * norm, 1.0))
    gain = square / (beta1 * beta1)
    length = gain * norm
    offset = mw - delta * mv - delta * (ww - delta * wv) - beta1 * beta1 * (wv - delta * vv)
    offset = gain * offset
    alpha2 = offset + shift * length
    c1 = -(delta + offset + shift * (length - 1.0))
    c2 = (alpha2 - shift) * delta - beta1 * beta1
    residual = mm + c1 * c1 * ww + c2 * c2 * vv + 2.0 * (c1 * mw + c2 * mv + c1 * c2 * wv)
    beta2 = jnp.sqrt(jnp.maximum(gain * residual, 1.0))
    factor = scale / (beta1 * beta2)
    return alpha1, alpha2, beta1, beta2, factor, factor * c1, factor * c2


def final_kernel(m, w, v, sigma, gram, out, scalars):
    @pl.when(pl.program_id(0) == 0)
    def _():
        row = lax.broadcasted_iota(jnp.int32, scalars.shape, 0)
        found = jnp.zeros(scalars.shape, jnp.float32)
        for k, value in enumerate(final_scalars(sigma, gram)):
            found = jnp.where(row == k, value, found)
        scalars[...] = found

    factor, c1, c2 = scalars[4:5, :], scalars[5:6, :], scalars[6:7, :]
    tile = m.shape[2]
    for k in range(m.shape[0]):
        at = slice(k * tile, (k + 1) * tile)
        value = factor * m[k].astype(jnp.float32) + c1 * w[k].astype(jnp.float32)
        out[:, at] = (value + c2 * v[:, at].astype(jnp.float32)).astype(jnp.bfloat16)


def finish_all(m, w, v, sigma, gram):
    rows, cols = v.shape
    tile = m.shape[2]
    column = pl.BlockSpec((tile, cols), lambda i: (i, 0))
    strip = pl.BlockSpec((cols // tile, tile, tile), lambda i: (0, i, 0))
    small = pl.BlockSpec((8, tile), lambda i: (0, 0))
    return pl.pallas_call(
        final_kernel,
        grid=(rows // tile,),
        in_specs=[strip, strip, column, small, small],
        out_specs=[column, small],
        out_shape=[
            jax.ShapeDtypeStruct((rows, cols), jnp.bfloat16),
            jax.ShapeDtypeStruct((8, tile), jnp.float32),
        ],
    )(m, w, v, sigma, gram)


def fused_body(start_vector, hop_tiles, tile_columns, tile_signs, occupation):
    rows, cols = start_vector.shape
    row_start = lax.axis_index("up") * rows
    col_start = lax.axis_index("dn") * cols
    occ = occupation.astype(jnp.bfloat16)
    occ_mine = lax.dynamic_slice_in_dim(occ, col_start, cols, 1)
    rows_t = lax.dynamic_slice_in_dim(occ, row_start, rows, 1).T
    cols_t = occ_mine.T
    m, w, sigma, gram = exchange(
        start_vector, hop_tiles, tile_columns.reshape(-1), tile_signs.reshape(-1),
        occ, occ_mine, rows_t, cols_t,
    )
    final, scalars = finish_all(m, w, start_vector, sigma, gram)
    return (final, scalars[0:2, 0], scalars[2:4, 0])


def fits(n_up, n_dn, rows, cols, tile):
    even = rows % (16 * n_dn) == 0 and cols % (16 * n_up) == 0
    return even and rows % tile == 0 and cols % (2 * tile) == 0


def chosen_body(start_vector, hop_tiles, *rest):
    rows, cols = start_vector.shape
    good = fits(lax.axis_size("up"), lax.axis_size("dn"), rows, cols, hop_tiles.shape[2])
    return (fused_body if good else body)(start_vector, hop_tiles, *rest)


def solution(mesh):
    placed = (P("up", "dn"), P(), P(), P(), P())
    return jax.shard_map(
        chosen_body, mesh=mesh, in_specs=placed, out_specs=(P("up", "dn"), P(), P()), check_vma=False
    )
```
